32 devices in a mesh: prow: 8 (over y, x, core), pcol: 4 (over z).
Axes of the slice: x: 2, y: 2, z: 4, core: 2. Of those that a mesh axis runs over, the one named last changes fastest.
Arguments:
- u_window: float32 [6, 8, 512, 4, 4, 512], P(None, 'prow', None, None, 'pcol'), may hold values from -0.625 to 0.625
Outputs:
- lauum_columns: float32 [1024, 6, 8, 512], P('pcol', None, 'prow')
The draws below stay inside these ranges and needn't reach their ends.
All inputs are finite; a program needn't handle non-finite values.
Results may differ from the reference program's by a relative error of at most 0.000061.
Values sent between devices are 32-bit elements; how exact they have to be, the bound alone decides.
No kernel may reach another device: no remote copies, remote signals or barrier semaphores. Data moves between devices by JAX's collectives and lax.ppermute only.
A program may use at most 192 MiB of HBM per device.

```python
import jax
import jax.numpy as jnp
from jax import lax

NB = 512
RB = 6
CB = 4
N_PROW = 8
N_PCOL = 4


def level_of(key, shape, split, least, top_value):
    gain, own = 1.0, jax.random.fold_in(key, 6)
    for axis_at, blocks in split:
        heights = jnp.exp(jax.random.uniform(jax.random.fold_in(own, axis_at), (blocks,), jnp.float32, least / len(split), top_value / len(split)))
        gain = gain * jnp.repeat(heights, shape[axis_at] // blocks).reshape([-1 if axis == axis_at else 1 for axis in range(len(shape))])
    return gain


def normal_values(key, dims, width, limit, cuts=(), held_as=jnp.bfloat16):
    values = width * jax.random.normal(key, dims, jnp.float32)
    if cuts:
        values = values * level_of(key, dims, cuts, -0.22, 0.18)
    return jnp.clip(values, -limit, limit).astype(held_as)


def setup_inputs(seed: int = 0) -> dict:
    splits = jax.random.split(jax.random.key(seed), 2)
    return {
        "u_window": normal_values(splits[0], (RB, N_PROW, NB, CB, N_PCOL, NB), ((CB * N_PCOL * NB) ** -0.25), 0.625, ((1, 8), (4, 4)), jnp.float32),
    }


def contract(left, right):
    return lax.dot_general(left, right, (((1,), (1,)), ((), ())), precision=lax.Precision.HIGHEST, preferred_element_type=jnp.float32)


def reference(u_window):
    height = RB * N_PROW
    width_cols = CB * N_PCOL * NB
    matrix = u_window.reshape(height * NB, width_cols)
    anchor = (height - 2) * NB
    panel_rows = matrix[anchor:]
    row_ids = jnp.arange(2 * NB, dtype=jnp.int32)
    col_ids = jnp.arange(width_cols, dtype=jnp.int32)
    masked = jnp.where(row_ids[:, None] <= col_ids[None, :], panel_rows, jnp.zeros_like(panel_rows))
    product = jnp.concatenate([contract(masked, matrix[:anchor]), contract(masked, masked)], 1)
    return product.reshape(2 * NB, RB, N_PROW, NB)
```

```python
import functools

import jax
import jax.numpy as jnp
from jax import lax
from jax.experimental import pallas as pl
from jax.experimental.pallas import tpu as pltpu
from jax.sharding import PartitionSpec as P

LANES = 128
CHUNKS = 4
PREP_ROWS = 256


def split(value):
    high = value.astype(jnp.bfloat16)
    low = (value - high.astype(jnp.float32)).astype(jnp.bfloat16)
    return high, low


def prep_kernel(place, source, high_ref, low_ref, *, block_size, last_start, anchor, prow_size, pcol_size):
    rows, width = high_ref.shape
    groups = width // LANES
    start = pl.program_id(0) * rows

    def emit(masked):
        for group in range(groups):
            value = source[pl.ds(group, rows, stride=groups), :]
            if masked:
                col = group * LANES
                base = (col // block_size * pcol_size + place[1]) * block_size + col % block_size
                first = (last_start // block_size * prow_size + place[0]) * block_size
                row_ids = first + start - last_start + lax.broadcasted_iota(jnp.int32, value.shape, 0)
                col_ids = anchor + base + lax.broadcasted_iota(jnp.int32, value.shape, 1)
                value = jnp.where(row_ids <= col_ids, value, 0.0)
            high, low = split(value)
            at = pl.ds(group * LANES, LANES)
            high_ref[:, at] = high
            low_ref[:, at] = low

    @pl.when(start < last_start)
    def _():
        emit(False)

    @pl.when(start >= last_start)
    def _():
        emit(True)


def dot(left, right):
    return lax.dot_general(
        left, right, (((1,), (1,)), ((), ())), preferred_element_type=jnp.float32
    )


def product_kernel(first, second, high_ref, low_ref, out_ref, left_high, left_low):
    half = out_ref.shape[0] // 2
    groups = left_high.shape[1] // LANES

    @pl.when(pl.program_id(0) == 0)
    def _():
        for index, panel in enumerate((first, second)):
            for group in range(groups):
                high, low = split(panel[pl.ds(group, half, stride=groups), :])
                at = (pl.ds(index * half, half), pl.ds(group * LANES, LANES))
                left_high[at] = high
                left_low[at] = low

    out_ref[...] = (
        dot(left_high[...], low_ref[...])
        + dot(left_low[...], high_ref[...])
        + dot(left_high[...], high_ref[...])
    )


def tree_steps(count, upward):
    spans = []
    span = 1
    while span < count:
        spans.append(span)
        span *= 2
    have = [0]
    steps = []
    for span in spans if upward else spans[::-1]:
        sends = [(at, at + span) for at in have if at + span < count and at + span not in have]
        have += [to for _, to in sends]
        steps.append([(count - 1 - at, count - 1 - to) for at, to in sends])
    return steps


def broadcast(kept, prow_size, my_row):
    pairs = prow_size // 2
    held = kept
    for even, odd in zip(tree_steps(pairs, True), tree_steps(pairs, False)):
        moves = [(2 * a, 2 * b) for a, b in even] + [(2 * a + 1, 2 * b + 1) for a, b in odd]
        landed = lax.ppermute(held, "prow", moves)
        targets = jnp.array([any(to == row for _, to in moves) for row in range(prow_size)])
        held = jnp.where(targets[my_row], landed, held)
    other = lax.ppermute(held, "prow", [(row, row ^ 1) for row in range(prow_size)])
    is_even = my_row % 2 == 0
    return jnp.where(is_even, held, other), jnp.where(is_even, other, held)


def on_device(u_window):
    row_blocks = u_window.shape[0]
    block_size = u_window.shape[2]
    col_blocks = u_window.shape[3]
    prow_size = lax.axis_size("prow")
    pcol_size = lax.axis_size("pcol")
    my_row = lax.axis_index("prow")
    my_col = lax.axis_index("pcol")
    width = col_blocks * block_size
    groups = width // LANES
    rows = row_blocks * block_size
    last_start = rows - block_size
    anchor = (row_blocks * prow_size - 2) * block_size
    lines = u_window.reshape(rows * groups, LANES)

    last = lines[last_start * groups :].reshape(block_size, groups, LANES)
    row_ids = ((row_blocks - 1) * prow_size + my_row) * block_size + jnp.arange(
        block_size, dtype=jnp.int32
    )
    col_index = jnp.arange(width, dtype=jnp.int32)
    window_col = (
        col_index // block_size * pcol_size + my_col
    ) * block_size + col_index % block_size
    keep = row_ids[:, None, None] <= anchor + window_col.reshape(1, groups, LANES)
    masked = jnp.where(keep, last, 0.0)
    shares = pcol_size // 2
    part = block_size // shares // CHUNKS
    pieces = masked.reshape(shares, CHUNKS, part, groups, LANES)
    panels = [
        broadcast(pieces[:, k].reshape(shares * part * groups, LANES), prow_size, my_row)
        for k in range(CHUNKS)
    ]

    place = jnp.stack([my_row, my_col]).astype(jnp.int32)
    half = jax.ShapeDtypeStruct((rows, width), jnp.bfloat16)
    high, low = pl.pallas_call(
        functools.partial(
            prep_kernel,
            block_size=block_size,
            last_start=last_start,
            anchor=anchor,
            prow_size=prow_size,
            pcol_size=pcol_size,
        ),
        grid=(rows // PREP_ROWS,),
        in_specs=[
            pl.BlockSpec(memory_space=pltpu.SMEM),
            pl.BlockSpec((PREP_ROWS * groups, LANES), lambda i: (i, 0)),
        ],
        out_specs=[pl.BlockSpec((PREP_ROWS, width), lambda i: (i, 0))] * 2,
        out_shape=[half, half],
        cost_estimate=pl.CostEstimate(
            flops=10 * rows * width, bytes_accessed=8 * rows * width, transcendentals=0
        ),
        name="prep",
    )(place, lines)

    chunk_rows = 2 * shares * part
    multiply = pl.pallas_call(
        product_kernel,
        grid=(row_blocks,),
        in_specs=[pl.BlockSpec((shares * part * groups, LANES), lambda i: (0, 0))] * 2
        + [pl.BlockSpec((block_size, width), lambda i: (i, 0))] * 2,
        out_specs=pl.BlockSpec((chunk_rows, block_size), lambda i: (0, i)),
        out_shape=jax.ShapeDtypeStruct((chunk_rows, rows), jnp.float32),
        scratch_shapes=[pltpu.VMEM((chunk_rows, width), jnp.bfloat16)] * 2,
        cost_estimate=pl.CostEstimate(
            flops=6 * chunk_rows * rows * width,
            bytes_accessed=4 * rows * width + 4 * chunk_rows * rows,
            transcendentals=0,
        ),
        name="product",
    )
    summed = [
        lax.psum_scatter(
            multiply(first, second, high, low), "pcol", scatter_dimension=0, tiled=True
        )
        for first, second in panels
    ]
    share = jnp.concatenate(summed, 0)
    return share.reshape(share.shape[0], row_blocks, 1, block_size)


def solution(mesh):
    placed = (P(None, "prow", None, None, "pcol", None),)
    return jax.shard_map(
        on_device,
        mesh=mesh,
        in_specs=placed,
        out_specs=P("pcol", None, "prow", None),
        check_vma=False,
    )
```

```python
import functools

import jax
import jax.numpy as jnp
from jax import lax
from jax.experimental import pallas as pl
from jax.experimental.pallas import tpu as pltpu
from jax.sharding import PartitionSpec as P


LANES = 128
SIXTEENTHS = (3, 5, 8)
PREP_ROWS = 256


def split(value):
    high = value.astype(jnp.bfloat16)
    low = (value - high.astype(jnp.float32)).astype(jnp.bfloat16)
    return high, low


def prep_kernel(
    place, source, *refs, begin, block_size, last_start, anchor, prow_size, pcol_size
):
    high_ref, low_ref = refs[-2:]
    rows, width = high_ref.shape
    groups = width // LANES
    start = begin + pl.program_id(0) * rows

    def emit(masked):
        for group in range(groups):
            value = source[pl.ds(group, rows, stride=groups), :]
            if masked:
                col = group * LANES
                base = (col // block_size * pcol_size + place[1]) * block_size + col % block_size
                first = (last_start // block_size * prow_size + place[0]) * block_size
                row_ids = first + start - last_start + lax.broadcasted_iota(jnp.int32, value.shape, 0)
                col_ids = anchor + base + lax.broadcasted_iota(jnp.int32, value.shape, 1)
                value = jnp.where(row_ids <= col_ids, value, 0.0)
            high, low = split(value)
            at = pl.ds(group * LANES, LANES)
            high_ref[:, at] = high
            low_ref[:, at] = low

    @pl.when(start < last_start)
    def _():
        emit(False)

    @pl.when(start >= last_start)
    def _():
        emit(True)


def dot(left, right):
    return lax.dot_general(
        left, right, (((1,), (1,)), ((), ())), preferred_element_type=jnp.float32
    )


def product_kernel(first, second, high_ref, low_ref, out_ref, left_high, left_low):
    half = left_high.shape[0] // 2
    groups = left_high.shape[1] // LANES
    block_size = high_ref.shape[0]
    lines = out_ref.shape[0] // left_high.shape[0]
    step = pl.program_id(0)

    @pl.when(pl.program_id(0) == 0)
    def _():
        for index, panel in enumerate((first, second)):
            for group in range(groups):
                high, low = split(panel[pl.ds(group, half, stride=groups), :])
                at = (pl.ds(index * half, half), pl.ds(group * LANES, LANES))
                left_high[at] = high
                left_low[at] = low

    result = (
        dot(left_high[...], low_ref[...])
        + dot(left_low[...], high_ref[...])
        + dot(left_high[...], high_ref[...])
    )
    spans = block_size // LANES
    for span in range(spans):
        out_ref[pl.ds(step * spans + span, 2 * half, stride=lines), :] = result[
            :, span * LANES : (span + 1) * LANES
        ]


def tree_steps(count, upward):
    spans = []
    span = 1
    while span < count:
        spans.append(span)
        span *= 2
    have = [0]
    steps = []
    for span in spans if upward else spans[::-1]:
        sends = [(at, at + span) for at in have if at + span < count and at + span not in have]
        have += [to for _, to in sends]
        steps.append([(count - 1 - at, count - 1 - to) for at, to in sends])
    return steps


def broadcast(kept, prow_size, my_row):
    pairs = prow_size // 2
    held = kept
    steps = zip(tree_steps(pairs, True), tree_steps(pairs, False))
    for even, odd in steps:
        moves = [(2 * a, 2 * b) for a, b in even] + [(2 * a + 1, 2 * b + 1) for a, b in odd]
        landed = lax.ppermute(held, "prow", moves)
        is_target = functools.reduce(jnp.logical_or, [my_row == to for _, to in moves])
        held = jnp.where(is_target, landed, held)
    other = lax.ppermute(held, "prow", [(row, row ^ 1) for row in range(prow_size)])
    is_even = my_row % 2 == 0
    return jnp.where(is_even, held, other), jnp.where(is_even, other, held)


def on_device(u_window):
    row_blocks = u_window.shape[0]
    block_size = u_window.shape[2]
    col_blocks = u_window.shape[3]
    prow_size = lax.axis_size("prow")
    pcol_size = lax.axis_size("pcol")
    my_row = lax.axis_index("prow")
    my_col = lax.axis_index("pcol")
    width = col_blocks * block_size
    groups = width // LANES
    rows = row_blocks * block_size
    last_start = rows - block_size
    anchor = (row_blocks * prow_size - 2) * block_size
    lines = u_window.reshape(rows * groups, LANES)

    last = lines[last_start * groups :].reshape(block_size, groups, LANES)
    row_ids = ((row_blocks - 1) * prow_size + my_row) * block_size + jnp.arange(
        block_size, dtype=jnp.int32
    )
    col_index = jnp.arange(width, dtype=jnp.int32)
    window_col = (
        col_index // block_size * pcol_size + my_col
    ) * block_size + col_index % block_size
    keep = row_ids[:, None, None] <= anchor + window_col.reshape(1, groups, LANES)
    masked = jnp.where(keep, last, 0.0)
    shares = pcol_size // 2
    share_rows = block_size // shares
    shaped = masked.reshape(shares, share_rows, groups, LANES)
    parts = [count * share_rows // sum(SIXTEENTHS) for count in SIXTEENTHS]
    panels = []
    at = 0
    for part in parts:
        piece = shaped[:, at : at + part].reshape(shares * part * groups, LANES)
        panels.append(broadcast(piece, prow_size, my_row))
        at += part

    place = jnp.stack([my_row, my_col]).astype(jnp.int32)
    halves = ()
    steps = rows // PREP_ROWS // 2
    for index in range(2):
        first_step = index * steps
        halves = pl.pallas_call(
            functools.partial(
                prep_kernel,
                begin=first_step * PREP_ROWS,
                block_size=block_size,
                last_start=last_start,
                anchor=anchor,
                prow_size=prow_size,
                pcol_size=pcol_size,
            ),
            grid=(steps,),
            in_specs=[
                pl.BlockSpec(memory_space=pltpu.SMEM),
                pl.BlockSpec((PREP_ROWS * groups, LANES), lambda i, base=first_step: (base + i, 0)),
            ]
            + [pl.BlockSpec(memory_space=pl.ANY)] * len(halves),
            out_specs=[pl.BlockSpec((PREP_ROWS, width), lambda i, base=first_step: (base + i, 0))]
            * 2,
            out_shape=[jax.ShapeDtypeStruct((rows, width), jnp.bfloat16)] * 2,
            input_output_aliases={2: 0, 3: 1} if halves else {},
            cost_estimate=pl.CostEstimate(
                flops=10 * rows * width, bytes_accessed=4 * rows * width, transcendentals=0
            ),
        )(place, lines, *halves)
    high, low = halves

    summed = []
    lines_out = rows // LANES
    for part, (first, second) in zip(parts, panels):
        chunk_rows = 2 * shares * part
        partial = pl.pallas_call(
            product_kernel,
            grid=(row_blocks,),
            in_specs=[pl.BlockSpec((shares * part * groups, LANES), lambda i: (0, 0))] * 2
            + [pl.BlockSpec((block_size, width), lambda i: (i, 0))] * 2,
            out_specs=pl.BlockSpec((chunk_rows * lines_out, LANES), lambda i: (0, 0)),
            out_shape=jax.ShapeDtypeStruct((chunk_rows * lines_out, LANES), jnp.float32),
            scratch_shapes=[pltpu.VMEM((chunk_rows, width), jnp.bfloat16)] * 2,
            cost_estimate=pl.CostEstimate(
                flops=6 * chunk_rows * rows * width,
                bytes_accessed=4 * rows * width + 4 * chunk_rows * rows,
                transcendentals=0,
            ),
        )(first, second, high, low)
        summed.append(lax.psum_scatter(partial, "pcol", scatter_dimension=0, tiled=True))
    return jnp.concatenate(summed, 0).reshape(2 * block_size // pcol_size, row_blocks, 1, block_size)


def solution(mesh):
    placed = (P(None, "prow", None, None, "pcol", None),)
    return jax.shard_map(
        on_device,
        mesh=mesh,
        in_specs=placed,
        out_specs=P("pcol", None, "prow", None),
        check_vma=False,
    )
```

```python
import functools

import jax
import jax.numpy as jnp
from jax import lax
from jax.experimental import pallas as pl
from jax.experimental.pallas import tpu as pltpu
from jax.sharding import PartitionSpec as P


LANES = 128
SIXTEENTHS = (3, 5, 8)
PREP_ROWS = 256


def split(value):
    high = value.astype(jnp.bfloat16)
    low = (value - high.astype(jnp.float32)).astype(jnp.bfloat16)
    return high, low


def prep_kernel(
    place, source, *refs, begin, block_size, last_start, anchor, prow_size, pcol_size
):
    high_ref, low_ref = refs[-2:]
    rows, width = high_ref.shape
    groups = width // LANES
    start = begin + pl.program_id(0) * rows

    def emit(masked):
        for group in range(groups):
            value = source[pl.ds(group, rows, stride=groups), :]
            if masked:
                col = group * LANES
                base = (col // block_size * pcol_size + place[1]) * block_size + col % block_size
                first = (last_start // block_size * prow_size + place[0]) * block_size
                row_ids = first + start - last_start + lax.broadcasted_iota(jnp.int32, value.shape, 0)
                col_ids = anchor + base + lax.broadcasted_iota(jnp.int32, value.shape, 1)
                value = jnp.where(row_ids <= col_ids, value, 0.0)
            high, low = split(value)
            at = pl.ds(group * LANES, LANES)
            high_ref[:, at] = high
            low_ref[:, at] = low

    @pl.when(start < last_start)
    def _():
        emit(False)

    @pl.when(start >= last_start)
    def _():
        emit(True)


def dot(left, right):
    return lax.dot_general(
        left, right, (((1,), (1,)), ((), ())), preferred_element_type=jnp.float32
    )


def product_kernel(first, second, high_ref, low_ref, out_ref, left):
    half = left.shape[0] // 4
    groups = left.shape[1] // LANES
    block_size = high_ref.shape[0]
    lines = out_ref.shape[0] // (2 * half)
    step = pl.program_id(0)

    @pl.when(pl.program_id(0) == 0)
    def _():
        for index, panel in enumerate((first, second)):
            for group in range(groups):
                high, low = split(panel[pl.ds(group, half, stride=groups), :])
                at = pl.ds(group * LANES, LANES)
                left[pl.ds(index * half, half), at] = high
                left[pl.ds((2 + index) * half, half), at] = low

    by_high = dot(left[...], high_ref[...])
    by_low = dot(left[: 2 * half], low_ref[...])
    result = by_low + by_high[2 * half :] + by_high[: 2 * half]
    spans = block_size // LANES
    for span in range(spans):
        out_ref[pl.ds(step * spans + span, 2 * half, stride=lines), :] = result[
            :, span * LANES : (span + 1) * LANES
        ]


def tree_steps(count, upward):
    spans = []
    span = 1
    while span < count:
        spans.append(span)
        span *= 2
    have = [0]
    steps = []
    for span in spans if upward else spans[::-1]:
        sends = [(at, at + span) for at in have if at + span < count and at + span not in have]
        have += [to for _, to in sends]
        steps.append([(count - 1 - at, count - 1 - to) for at, to in sends])
    return steps


def broadcast(kept, prow_size, my_row):
    pairs = prow_size // 2
    held = kept
    steps = zip(tree_steps(pairs, True), tree_steps(pairs, False))
    for even, odd in steps:
        moves = [(2 * a, 2 * b) for a, b in even] + [(2 * a + 1, 2 * b + 1) for a, b in odd]
        landed = lax.ppermute(held, "prow", moves)
        is_target = functools.reduce(jnp.logical_or, [my_row == to for _, to in moves])
        held = jnp.where(is_target, landed, held)
    other = lax.ppermute(held, "prow", [(row, row ^ 1) for row in range(prow_size)])
    is_even = my_row % 2 == 0
    return jnp.where(is_even, held, other), jnp.where(is_even, other, held)


def on_device(u_window):
    row_blocks = u_window.shape[0]
    block_size = u_window.shape[2]
    col_blocks = u_window.shape[3]
    prow_size = lax.axis_size("prow")
    pcol_size = lax.axis_size("pcol")
    my_row = lax.axis_index("prow")
    my_col = lax.axis_index("pcol")
    width = col_blocks * block_size
    groups = width // LANES
    rows = row_blocks * block_size
    last_start = rows - block_size
    anchor = (row_blocks * prow_size - 2) * block_size
    lines = u_window.reshape(rows * groups, LANES)

    last = lines[last_start * groups :].reshape(block_size, groups, LANES)
    row_ids = ((row_blocks - 1) * prow_size + my_row) * block_size + jnp.arange(
        block_size, dtype=jnp.int32
    )
    col_index = jnp.arange(width, dtype=jnp.int32)
    window_col = (
        col_index // block_size * pcol_size + my_col
    ) * block_size + col_index % block_size
    keep = row_ids[:, None, None] <= anchor + window_col.reshape(1, groups, LANES)
    masked = jnp.where(keep, last, 0.0)
    shares = pcol_size // 2
    share_rows = block_size // shares
    shaped = masked.reshape(shares, share_rows, groups, LANES)
    parts = [count * share_rows // sum(SIXTEENTHS) for count in SIXTEENTHS]
    panels = []
    at = 0
    for part in parts:
        piece = shaped[:, at : at + part].reshape(shares * part * groups, LANES)
        panels.append(broadcast(piece, prow_size, my_row))
        at += part

    place = jnp.stack([my_row, my_col]).astype(jnp.int32)
    halves = ()
    steps = rows // PREP_ROWS // 2
    for index in range(2):
        first_step = index * steps
        halves = pl.pallas_call(
            functools.partial(
                prep_kernel,
                begin=first_step * PREP_ROWS,
                block_size=block_size,
                last_start=last_start,
                anchor=anchor,
                prow_size=prow_size,
                pcol_size=pcol_size,
            ),
            grid=(steps,),
            in_specs=[
                pl.BlockSpec(memory_space=pltpu.SMEM),
                pl.BlockSpec((PREP_ROWS * groups, LANES), lambda i, base=first_step: (base + i, 0)),
            ]
            + [pl.BlockSpec(memory_space=pl.ANY)] * len(halves),
            out_specs=[pl.BlockSpec((PREP_ROWS, width), lambda i, base=first_step: (base + i, 0))]
            * 2,
            out_shape=[jax.ShapeDtypeStruct((rows, width), jnp.bfloat16)] * 2,
            input_output_aliases={2: 0, 3: 1} if halves else {},
            cost_estimate=pl.CostEstimate(
                flops=10 * rows * width, bytes_accessed=4 * rows * width, transcendentals=0
            ),
        )(place, lines, *halves)
    high, low = halves

    summed = []
    lines_out = rows // LANES
    for part, (first, second) in zip(parts, panels):
        chunk_rows = 2 * shares * part
        partial = pl.pallas_call(
            product_kernel,
            grid=(row_blocks,),
            in_specs=[pl.BlockSpec((shares * part * groups, LANES), lambda i: (0, 0))] * 2
            + [pl.BlockSpec((block_size, width), lambda i: (i, 0))] * 2,
            out_specs=pl.BlockSpec((chunk_rows * lines_out, LANES), lambda i: (0, 0)),
            out_shape=jax.ShapeDtypeStruct((chunk_rows * lines_out, LANES), jnp.float32),
            scratch_shapes=[pltpu.VMEM((2 * chunk_rows, width), jnp.bfloat16)],
            cost_estimate=pl.CostEstimate(
                flops=6 * chunk_rows * rows * width,
                bytes_accessed=4 * rows * width + 4 * chunk_rows * rows,
                transcendentals=0,
            ),
        )(first, second, high, low)
        summed.append(lax.psum_scatter(partial, "pcol", scatter_dimension=0, tiled=True))
    return jnp.concatenate(summed, 0).reshape(2 * block_size // pcol_size, row_blocks, 1, block_size)


def solution(mesh):
    placed = (P(None, "prow", None, None, "pcol", None),)
    return jax.shard_map(
        on_device,
        mesh=mesh,
        in_specs=placed,
        out_specs=P("pcol", None, "prow", None),
        check_vma=False,
    )
```
